128 devices in a mesh: fsdp: 16 (over y, x_hi, core), tp: 8 (over z, x_lo).
Axes of the slice: x: 4 (x_hi: 2, x_lo: 2; x = x_hi * 2 + x_lo), y: 4, z: 4, core: 2. Of those that a mesh axis runs over, the one named last changes fastest.
Arguments:
- w_gate: float32 [3072, 8192], P('fsdp', 'tp'), may hold values from -0.15625 to 0.15625
- first_gate: float32 [3072, 8192], P('fsdp', 'tp'), may hold values from -0.109375 to 0.109375
- second_gate: float32 [3072, 8192], P('fsdp', 'tp'), may hold values from -0.109375 to 0.109375
- w_up: float32 [3072, 8192], P('fsdp', 'tp'), may hold values from -0.15625 to 0.15625
- first_up: float32 [3072, 8192], P('fsdp', 'tp'), may hold values from -0.109375 to 0.109375
- second_up: float32 [3072, 8192], P('fsdp', 'tp'), may hold values from -0.109375 to 0.109375
- norm_train: float32 [3072], P(('fsdp', 'tp')), may hold values from 0.25 to 1.75
- norm_step: float32 [3072], P(('fsdp', 'tp')), may hold values from -0.3 to 0.3
Outputs:
- serving_gate: bfloat16 [3072, 8192], P(None, 'tp')
- serving_up: bfloat16 [3072, 8192], P(None, 'tp')
- scale_gate: float32 [8192], P('tp')
- scale_up: float32 [8192], P('tp')
- serve_norm: bfloat16 [3072], replicated
- whole_gate: float32 [3072, 8192], P('fsdp', 'tp')
- whole_up: float32 [3072, 8192], P('fsdp', 'tp')
The draws below stay inside these ranges and needn't reach their ends.
All inputs are finite; a program needn't handle non-finite values. Where the reference program divides by a largest or mean magnitude, that divisor is 1e-20 or more.
Results may differ from the reference program's by a relative error of at most 0.001.
Values may be sent and summed in bfloat16 or wider, within the bound.
No kernel may reach another device: no remote copies, remote signals or barrier semaphores. Data moves between devices by JAX's collectives and lax.ppermute only.
A program may use at most 128 MiB of HBM per device.

```python
import jax
import jax.numpy as jnp

D_MODEL = 3072
D_INNER = 8192


def spiked(entries, rng, source, target, shards_of, factor):
    owner, partner = [(jnp.arange(entries.shape[axis_at]) // (entries.shape[axis_at] // shards_of)).reshape([-1 if axis == axis_at else 1 for axis in range(entries.ndim)]) for axis_at in (source, target)]
    chosen = jax.random.permutation(rng, shards_of)[partner]
    strong = (owner == chosen) | (owner == (partner + shards_of // 2) % shards_of)
    return jnp.where(strong, factor * entries, entries)


def levels(own_key, extent, cuts, least, top_value):
    def one(position, shards_of):
        draws = jax.random.uniform(jax.random.fold_in(jax.random.fold_in(own_key, 6), position), (shards_of,), jnp.float32, least / len(cuts), top_value / len(cuts))
        return jnp.repeat(jnp.exp(draws), extent[position] // shards_of).reshape((-1,) + (1,) * (len(extent) - position - 1))

    loudness = one(*cuts[0])
    for cut in cuts[1:]:
        loudness = loudness * one(*cut)
    return loudness


def noise(rng, dims, width, bound, split=(), held_as=jnp.bfloat16):
    values = width * jax.random.normal(rng, dims, jnp.float32)
    if split:
        values = values * levels(rng, dims, split, -0.22, 0.18)
    return jnp.clip(values, -bound, bound).astype(held_as)


def bell_draw_with(key, shape, deviation, reach, pieces, heavy, dtype=jnp.bfloat16):
    result = deviation * jax.random.normal(key, shape, jnp.float32)
    if pieces:
        result = result * levels(key, shape, pieces, -0.22, 0.18)
    return jnp.clip(spiked(result, jax.random.fold_in(key, 3), *heavy), -reach, reach).astype(dtype)


def setup_inputs(seed: int = 0) -> dict:
    arg_keys = jax.random.split(jax.random.key(seed), 9)
    return {
        "w_gate": bell_draw_with(arg_keys[0], (D_MODEL, D_INNER), D_MODEL ** -0.5, 0.15625, ((0, 16), (1, 8)), (0, 1, 16, 2.0), jnp.float32),
        "first_gate": noise(arg_keys[1], (D_MODEL, D_INNER), D_MODEL ** -0.5, 0.109375, ((0, 16), (1, 8)), jnp.float32),
        "second_gate": noise(arg_keys[2], (D_MODEL, D_INNER), D_MODEL ** -0.5, 0.109375, ((0, 16), (1, 8)), jnp.float32),
        "w_up": bell_draw_with(arg_keys[3], (D_MODEL, D_INNER), D_MODEL ** -0.5, 0.15625, ((0, 16), (1, 8)), (0, 1, 16, 2.0), jnp.float32),
        "first_up": noise(arg_keys[4], (D_MODEL, D_INNER), D_MODEL ** -0.5, 0.109375, ((0, 16), (1, 8)), jnp.float32),
        "second_up": noise(arg_keys[5], (D_MODEL, D_INNER), D_MODEL ** -0.5, 0.109375, ((0, 16), (1, 8)), jnp.float32),
        "norm_train": jnp.clip(1.0 + 0.15 * jax.random.normal(arg_keys[6], (D_MODEL,), jnp.float32), 0.25, 1.75),
        "norm_step": jnp.clip(jax.random.uniform(arg_keys[7], (D_MODEL,), jnp.float32, -0.3, 0.3) * levels(arg_keys[7], (D_MODEL,), ((0, 128),), -0.4, 0.0), -0.3, 0.3),
    }


learn_rate = 0.25
hold_rate = 0.9


def reference(w_gate, first_gate, second_gate, w_up, first_up, second_up, norm_train, norm_step):
    hold_gate = hold_rate * first_gate + second_gate
    whole_gate = w_gate - learn_rate * hold_gate
    hold_up = hold_rate * first_up + second_up
    whole_up = w_up - learn_rate * hold_up
    scale_gate = jnp.sum(jnp.abs(whole_gate), axis=0) / D_MODEL
    serving_gate = (whole_gate / scale_gate).astype(jnp.bfloat16)
    scale_up = jnp.sum(jnp.abs(whole_up), axis=0) / D_MODEL
    serving_up = (whole_up / scale_up).astype(jnp.bfloat16)
    serve_norm = (norm_train + norm_step).astype(jnp.bfloat16)
    return serving_gate, serving_up, scale_gate, scale_up, serve_norm, whole_gate, whole_up
```

```python
import jax
import jax.numpy as jnp
from jax import lax
from jax.sharding import PartitionSpec as P

D_MODEL = 3072

learn_rate = 0.25
hold_rate = 0.9


Y, H, CORES = 4, 2, 2


def up(x):
    return lax.ppermute(x, "fsdp", [(f, (f + 4) % 16) for f in range(16)])


def down(x):
    return lax.ppermute(x, "fsdp", [(f, (f - 4) % 16) for f in range(16)])


def across(x):
    return lax.ppermute(x, "fsdp", [(f, f ^ 2) for f in range(16)])


def partner(x):
    return lax.ppermute(x, "fsdp", [(f, f ^ 1) for f in range(16)])


def gather_blocks(g, u):
    have = {(0, 0, "g"): g, (0, 0, "u"): u}
    order = []

    def send(link, key):
        dy, dh, part = key
        x = have[key]
        if link == "+":
            new = ((dy - 1) % 4, dh, part)
            have[new] = up(x)
        elif link == "-":
            new = ((dy + 1) % 4, dh, part)
            have[new] = down(x)
        else:
            new = (dy, 1 - dh, part)
            have[new] = across(x)
        order.append(new)

    send("+", (0, 0, "g"))
    send("-", (0, 0, "u"))
    send("x", (0, 0, "g"))
    send("+", (0, 0, "u"))
    send("-", (0, 0, "g"))
    send("x", (0, 0, "u"))
    send("+", (3, 0, "g"))
    send("-", (1, 0, "u"))
    send("+", (0, 1, "g"))
    send("-", (0, 1, "g"))
    send("x", (2, 0, "g"))
    send("x", (2, 0, "u"))
    send("+", (0, 1, "u"))
    send("-", (0, 1, "u"))
    blocks = {}
    for key in [(0, 0, "g"), (0, 0, "u")] + order:
        blocks[key + (0,)] = have[key]
        blocks[key + (1,)] = partner(have[key])
    return blocks


def exchange(shard):
    return lax.all_to_all(
        jnp.broadcast_to(shard[None, None], (16, 1, shard.shape[0])), "fsdp", 0, 0, tiled=True
    )[:, 0]


def norm_everywhere(mine):
    t = lax.axis_index("tp")
    held = mine[:, None, :]
    for bit in (1, 2, 4):
        other = lax.ppermute(held, "tp", [(i, i ^ bit) for i in range(8)])
        low = (t & bit) == 0
        held = jnp.concatenate(
            [jnp.where(low, held, other), jnp.where(low, other, held)], axis=1
        )
    return held.reshape(-1)


def per_device(w_gate, first_gate, second_gate, w_up, first_up, second_up, norm_train, norm_step):
    whole_gate = w_gate - learn_rate * (hold_rate * first_gate + second_gate)
    whole_up = w_up - learn_rate * (hold_rate * first_up + second_up)
    sums = jnp.concatenate(
        [
            jnp.sum(jnp.abs(whole_gate), axis=0),
            jnp.sum(jnp.abs(whole_up), axis=0),
            norm_train + norm_step,
            jnp.zeros((104,), jnp.float32),
        ]
    )
    everyone = exchange(sums)
    scales = jnp.sum(everyone[:, :2048], axis=0) / D_MODEL
    scale_gate, scale_up = scales[:1024], scales[1024:]
    serve_norm = norm_everywhere(everyone[:, 2048:2072].astype(jnp.bfloat16))
    g = (whole_gate / scale_gate).astype(jnp.bfloat16)
    u = (whole_up / scale_up).astype(jnp.bfloat16)
    blocks = gather_blocks(g, u)
    f = lax.axis_index("fsdp")
    y, h, c = f // 4, (f // 2) % 2, f % 2
    outs = {part: jnp.zeros((D_MODEL, 1024), jnp.bfloat16) for part in "gu"}
    for (dy, dh, part, dc), block in blocks.items():
        row = (((y + dy) % 4) * 4 + (h ^ dh) * 2 + (c ^ dc)) * 192
        outs[part] = lax.dynamic_update_slice(outs[part], block, (row, 0))
    return (outs["g"], outs["u"], scale_gate, scale_up, serve_norm, whole_gate, whole_up)


def solution(mesh):
    return jax.shard_map(
        per_device,
        mesh=mesh,
        in_specs=(P("fsdp", "tp"),) * 6 + (P(("fsdp", "tp")),) * 2,
        out_specs=(
            P(None, "tp"),
            P(None, "tp"),
            P("tp"),
            P("tp"),
            P(),
            P("fsdp", "tp"),
            P("fsdp", "tp"),
        ),
        check_vma=False,
    )
```
